32 devices in a mesh: heads: 2 (over x), tokens: 16 (over z, y, core).
Axes of the slice: x: 2, y: 2, z: 4, core: 2. Of those that a mesh axis runs over, the one named last changes fastest.
Arguments:
- queries: bfloat16 [128, 16, 576], P('heads', 'tokens'), may hold values from -40 to 40
- latent_keys: bfloat16 [16384, 576], P('tokens'), may hold values from -4 to 4
- index_queries: bfloat16 [16, 64, 128], P(None, 'heads'), may hold values from -4 to 4
- index_keys: bfloat16 [16384, 128], P('tokens'), may hold values from -8 to 8
- index_weights: float32 [16, 64], P(None, 'heads'), may hold values from 0 to 1.2
- positions: int32 [16], replicated, may hold values from 8192 to 16383
Outputs:
- index_query_grad: float32 [16, 64, 128], P(None, 'heads')
- index_weight_grad: float32 [16, 64], P(None, 'heads')
- index_key_grad: float32 [16384, 128], P('tokens')
The draws below stay inside these ranges and needn't reach their ends.
All inputs are finite; a program needn't handle non-finite values.
Results may differ from the reference program's by a relative error of at most 0.0026.
Values may be sent and summed in bfloat16 or wider, within the bound.
A program may use at most 64 MiB of HBM per device.

```python
import jax
import jax.numpy as jnp
from jax import lax

H = 128
DL = 512
DR = 64
HI = 64
DI = 128
Q = 16
KEYS = 16384
GRAD_SCALE = 2048


def main_pair(key):
    folded = jax.random.fold_in(key, 11)
    first_key, second_key = jax.random.split(folded, 2)
    width = DL + DR
    query_spread = 2.5 * (192.0 / width) ** 0.5
    key_rows = jnp.clip(jax.random.normal(first_key, (KEYS, width), jnp.float32), -4.0, 4.0)
    query_rows = query_spread * jnp.clip(jax.random.normal(second_key, (H, Q, width), jnp.float32), -4.0, 4.0)
    return (query_rows, key_rows)


def index_pair(key):
    folded = jax.random.fold_in(key, 23)
    first_key, second_key = jax.random.split(folded, 2)
    key_rows = jnp.clip(jax.random.normal(first_key, (KEYS, DI), jnp.float32), -4.0, 4.0)
    query_rows = jnp.clip(jax.random.normal(second_key, (Q, HI, DI), jnp.float32), -4.0, 4.0)
    key_rows = 0.7 * key_rows
    return (query_rows, key_rows)


def draw_queries(key, part):
    return main_pair(key)[0].astype(jnp.bfloat16)


def draw_latent_keys(key, part):
    return main_pair(key)[1].astype(jnp.bfloat16)


def draw_index_queries(key, part):
    return index_pair(key)[0].astype(jnp.bfloat16)


def draw_index_keys(key, part):
    return index_pair(key)[1].astype(jnp.bfloat16)


def touch_ends(drawn, key, smallest, high):
    longest = drawn.shape.index(max(drawn.shape))
    spots = []
    for shift in (0, 1):
        where = [jax.random.randint(jax.random.fold_in(key, axis), (), 0, length) for axis, length in enumerate(drawn.shape)]
        where[longest] = (where[longest] + shift) % drawn.shape[longest]
        spots.append(tuple(where))
    return drawn.at[spots[0]].set(smallest).at[spots[1]].set(high)


def block_scale(stream_key, extent, shards, smallest, high):
    def one(dim, blocks):
        heights = jax.random.uniform(jax.random.fold_in(jax.random.fold_in(stream_key, 6), dim), (blocks,), jnp.float32, smallest / len(shards), high / len(shards))
        return jnp.repeat(jnp.exp(heights), extent[dim] // blocks).reshape((-1,) + (1,) * (len(extent) - dim - 1))

    level = one(*shards[0])
    for cut in shards[1:]:
        level = level * one(*cut)
    return level


def setup_inputs(seed: int = 0) -> dict:
    key_of = jax.random.split(jax.random.key(seed), 7)
    queries = draw_queries(jax.random.fold_in(key_of[6], 71), 0)
    latent_keys = draw_latent_keys(jax.random.fold_in(key_of[6], 71), 0)
    index_queries = draw_index_queries(jax.random.fold_in(key_of[6], 71), 0)
    index_keys = draw_index_keys(jax.random.fold_in(key_of[6], 71), 0)
    index_weights = jnp.clip(1.2 * jax.random.uniform(key_of[4], (Q, HI), jnp.float32) ** block_scale(key_of[4], (Q, HI), ((1, 2),), -0.2, 0.2), 0.0, 1.2)
    positions = touch_ends(jax.random.randint(key_of[5], (Q,), KEYS // 2, KEYS), jax.random.fold_in(key_of[5], 1), KEYS // 2, KEYS - 1).astype(jnp.int32)
    return {"queries": queries, "latent_keys": latent_keys, "index_queries": index_queries, "index_keys": index_keys, "index_weights": index_weights, "positions": positions}


softmax_scale = 192.0 ** -0.5
masked_value = -1.0e30


def reference(queries, latent_keys, index_queries, index_keys, index_weights, positions):
    key_index = jnp.arange(KEYS, dtype=jnp.int32)
    visible = key_index[None, :] <= positions[:, None]

    def head_step(running, head_query):
        scores = jnp.dot(head_query, latent_keys.T, preferred_element_type=jnp.float32) * softmax_scale
        scores = jnp.where(visible, scores, masked_value)
        row_max = jnp.max(scores, axis=1, keepdims=True)
        exponent = jnp.exp(scores - row_max)
        row_sum = jnp.sum(exponent, axis=1, keepdims=True)
        return running + exponent / row_sum, None

    summed, _ = lax.scan(head_step, jnp.zeros((Q, KEYS), jnp.float32), queries)
    target = summed / H

    index_scale = DI ** -0.5
    head_queries = jnp.transpose(index_queries, (1, 0, 2))
    head_weights = index_weights.T

    def index_step(running, head_pair):
        head_query, head_weight = head_pair
        active = jnp.dot(head_query, index_keys.T, preferred_element_type=jnp.float32) * index_scale
        return running + head_weight[:, None] * jnp.maximum(active, 0.0), None

    logits, _ = lax.scan(index_step, jnp.zeros((Q, KEYS), jnp.float32), (head_queries, head_weights))
    logits = jnp.where(visible, logits, masked_value)
    row_max = jnp.max(logits, axis=1, keepdims=True)
    exponent = jnp.exp(logits - row_max)
    index_probs = exponent / jnp.sum(exponent, axis=1, keepdims=True)
    dlogit = GRAD_SCALE * (index_probs - target)

    def grad_step(running, head_pair):
        head_query, head_weight = head_pair
        active = jnp.dot(head_query, index_keys.T, preferred_element_type=jnp.float32) * index_scale
        gate_grad = (dlogit * head_weight[:, None] * (active > 0.0)).astype(jnp.bfloat16)
        query_grad = jnp.dot(gate_grad, index_keys, preferred_element_type=jnp.float32) * index_scale
        weight_grad = jnp.sum(dlogit * jnp.maximum(active, 0.0), axis=1)
        key_grad = running + jnp.dot(gate_grad.T, head_query, preferred_element_type=jnp.float32) * index_scale
        return key_grad, (query_grad, weight_grad)

    key_grad, (query_grads, weight_grads) = lax.scan(grad_step, jnp.zeros((KEYS, DI), jnp.float32), (head_queries, head_weights))
    return jnp.transpose(query_grads, (1, 0, 2)), weight_grads.T, key_grad
```

```python
import functools

import jax
import jax.numpy as jnp
from jax import lax
from jax.experimental import pallas as pl
from jax.experimental.pallas import tpu as pltpu
from jax.sharding import PartitionSpec as P

MESH = pl.DeviceIdType.MESH
softmax_scale = 192.0 ** (-0.5)
masked_value = -1e30
open_value = 3e38
f32 = jnp.float32
bf16 = jnp.bfloat16


def swapped(value, step, size):
    if size & (size - 1):
        return lax.rem(value + step, size)
    out = value
    bit = 1
    while bit < size:
        if step & bit:
            out = out + bit - 2 * bit * lax.rem(lax.div(value, bit), 2)
        bit *= 2
    return out


def as_row(column, eye):
    return jnp.sum(jnp.where(eye, column, 0.0), axis=0, keepdims=True)


def eye_of(rows):
    return lax.broadcasted_iota(jnp.int32, (rows, 128), 0) == lax.broadcasted_iota(jnp.int32, (rows, 128), 1)


def kernel(
    cfg, q_in, k_in, iq_in, ik_in, w_in, pos_ref, qg_out, kg_out,
    qbuf, kbuf, iqbuf, ikbuf, wbuf, wcol, p, act, gate, ml, mrow, colm, coll, stats, istats, tbuf, dbuf,
    qpart, pairbuf, rsend, rsbuf, agbuf,
    lsem, zs, ys, cs, qr, hs, hr, ws, wr, ss, sr, iss, isr, ts, tr, ps, pr, rs, rr, gs, gr,
):
    NH, N, Z, Y, Q, R, D, Kl, Jl, SL, H, loss_scale = cfg
    G = 2 * Y
    NC = N // 2
    me = lax.axis_index("tokens")
    mh = lax.axis_index("heads")
    core = lax.rem(me, 2)
    chip = lax.div(me, 2)
    y = lax.rem(chip, Y)
    z = lax.div(chip, Y)
    partner = me + 1 - 2 * core

    def at(zz, yy, cc):
        return (zz * Y + yy) * 2 + cc

    def remote(src, dst, send, recv, tok=None, head=None):
        device = {"tokens": tok} if head is None else {"heads": head}
        return pltpu.make_async_remote_copy(
            src_ref=src, dst_ref=dst, send_sem=send, recv_sem=recv, device_id=device, device_id_type=MESH
        )

    loads = [
        pltpu.make_async_copy(q_in, qbuf.at[me], lsem.at[0]),
        pltpu.make_async_copy(iq_in, iqbuf.at[mh], lsem.at[1]),
        pltpu.make_async_copy(w_in, wbuf.at[mh], lsem.at[2]),
        pltpu.make_async_copy(ik_in, ikbuf, lsem.at[3]),
        pltpu.make_async_copy(k_in, kbuf, lsem.at[4]),
    ]
    for load in loads:
        load.start()
    barrier = pltpu.get_barrier_semaphore()
    for i in range(1, N):
        pl.semaphore_signal(barrier, inc=1, device_id={"tokens": lax.rem(me + i, N)}, device_id_type=MESH)
    for i in range(1, NH):
        pl.semaphore_signal(barrier, inc=1, device_id={"heads": lax.rem(mh + i, NH)}, device_id_type=MESH)
    for load in loads[:3]:
        load.wait()
    pl.semaphore_wait(barrier, N - 1 + NH - 1)

    sends = []

    def go(copy):
        copy.start()
        sends.append(copy)

    def send_query(src, sem, dest):
        go(remote(qbuf.at[src], qbuf.at[src], sem, qr.at[src], tok=dest))

    def await_query(src):
        remote(qbuf.at[src], qbuf.at[src], zs.at[0], qr.at[src], tok=partner).wait_recv()

    for i in range(1, Z):
        send_query(me, zs.at[i], at(swapped(z, i, Z), y, core))
    for j in range(1, Y):
        send_query(me, ys.at[j], at(z, swapped(y, j, Y), core))
    send_query(me, cs.at[0], partner)
    for i in range(1, NH):
        other = lax.rem(mh + i, NH)
        go(remote(iqbuf.at[mh], iqbuf.at[mh], hs.at[i], hr.at[mh], head=other))
        go(remote(wbuf.at[mh], wbuf.at[mh], ws.at[i], wr.at[mh], head=other))

    key_index = me * Kl + lax.broadcasted_iota(jnp.int32, (1, Kl), 1)
    iscale = 128.0 ** (-0.5)

    def index_part(h):
        wt = jnp.transpose(wbuf[h])
        for t in range(Q):
            wcol[h, t * Jl : (t + 1) * Jl, :] = jnp.broadcast_to(wt[:, t : t + 1], (Jl, 128))
        act[h] = (
            lax.dot_general(iqbuf[h], ikbuf[...], (((1,), (1,)), ((), ())), preferred_element_type=f32) * iscale
        )

    def index_logits(h, first):
        def body(o, carry):
            parts = [[] for _ in range(Kl // 128)]
            for u in range(8):
                rows = pl.ds(pl.multiple_of((o * 8 + u) * Jl, 8), Jl)
                wc = wcol[h, rows, :]
                for lt in range(Kl // 128):
                    a = jnp.maximum(act[h, rows, lt * 128 : (lt + 1) * 128], 0.0)
                    parts[lt].append(jnp.sum(a * wc, axis=0, keepdims=True))
            eight = pl.ds(pl.multiple_of(o * 8, 8), 8)
            for lt in range(Kl // 128):
                lanes = slice(lt * 128, (lt + 1) * 128)
                part = jnp.concatenate(parts[lt], axis=0)
                ml[eight, lanes] = part if first else ml[eight, lanes] + part
            return carry

        lax.fori_loop(0, Q // 8, body, 0)

    eye128 = eye_of(128)

    def score_group(zg):
        group = qbuf[pl.ds(zg * G, G)].reshape(G * R, D)
        base = zg * (G * R)
        scores = lax.dot_general(group, kbuf[...], (((1,), (1,)), ((), ())), preferred_element_type=f32)
        step = min(32, R)
        for i in range(G):
            cap = jnp.where(key_index <= pos_ref[zg * G + i], open_value, masked_value)
            for r in range(0, R, step):
                row = i * R + r
                s = jnp.minimum(scores[row : row + step] * softmax_scale, cap)
                m = jnp.max(s, axis=1, keepdims=True)
                e = jnp.exp(s - m)
                p[pl.ds(pl.multiple_of(base + row, 8), step), :] = e
                colm[row : row + step, :] = m
                coll[row : row + step, :] = m + jnp.log(jnp.sum(e, axis=1, keepdims=True))
        for b in range(G * R // 128):
            mrow[zg, b : b + 1, :] = as_row(colm[b * 128 : (b + 1) * 128, :], eye128)
            stats[me, zg, b : b + 1, :] = as_row(coll[b * 128 : (b + 1) * 128, :], eye128)

    loads[3].wait()
    for i in range(NH):
        h = lax.rem(mh + i, NH)
        if i > 0:
            remote(iqbuf.at[h], iqbuf.at[h], hs.at[0], hr.at[h], head=lax.rem(mh + 1, NH)).wait_recv()
            remote(wbuf.at[h], wbuf.at[h], ws.at[0], wr.at[h], head=lax.rem(mh + 1, NH)).wait_recv()
        index_part(h)
        index_logits(h, i == 0)
        if i == 0:
            loads[4].wait()
            for j in range(1, Y):
                src = at(z, swapped(y, j, Y), core)
                await_query(src)
                send_query(src, cs.at[j], partner)
            for j in range(Y):
                await_query(at(z, swapped(y, j, Y), 1 - core))

    cap = jnp.concatenate([jnp.where(key_index <= pos_ref[t], open_value, masked_value) for t in range(Q)], axis=0)
    logits = jnp.minimum(ml[...], cap)
    ml[...] = logits
    imax = jnp.max(logits, axis=1, keepdims=True)
    isum = jnp.sum(jnp.exp(logits - imax), axis=1, keepdims=True)
    eyeq = eye_of(Q)
    istats[me, 0:1, :] = as_row(imax, eyeq)
    istats[me, 1:2, :] = as_row(isum, eyeq)
    for i in range(1, N):
        dst = lax.rem(me + i, N)
        go(remote(istats.at[me], istats.at[me], iss.at[i], isr.at[me], tok=dst))

    for i in range(1, Z):
        zz = swapped(z, i, Z)
        src = at(zz, y, core)
        await_query(src)
        for j in range(1, Y):
            send_query(src, ys.at[i * Y + j], at(z, swapped(y, j, Y), core))
        send_query(src, cs.at[i * Y], partner)
        score_group(swapped(z, i - 1, Z))
        for j in range(1, Y):
            src = at(zz, swapped(y, j, Y), core)
            await_query(src)
            send_query(src, cs.at[i * Y + j], partner)
        for j in range(Y):
            await_query(at(zz, swapped(y, j, Y), 1 - core))
    score_group(swapped(z, Z - 1, Z))

    for i in range(1, N):
        dst = lax.rem(me + i, N)
        go(remote(stats.at[me], stats.at[me], ss.at[i], sr.at[me], tok=dst))
    for i in range(1, N):
        src = lax.rem(me + i, N)
        remote(istats.at[src], istats.at[src], iss.at[0], isr.at[src], tok=partner).wait_recv()
    gmax = functools.reduce(jnp.maximum, [istats[i, 0:1, :] for i in range(N)])
    gsum = functools.reduce(jnp.add, [istats[i, 1:2, :] * jnp.exp(istats[i, 0:1, :] - gmax) for i in range(N)])
    gmax_col = jnp.sum(jnp.where(eyeq, gmax, 0.0), axis=1, keepdims=True)
    gsum_col = jnp.sum(jnp.where(eyeq, gsum, 0.0), axis=1, keepdims=True)
    dbuf[...] = jnp.exp(ml[...] - gmax_col) / gsum_col
    for i in range(1, N):
        src = lax.rem(me + i, N)
        remote(stats.at[src], stats.at[src], ss.at[0], sr.at[src], tok=partner).wait_recv()
    smax = functools.reduce(jnp.maximum, [stats[i] for i in range(N)])
    ssum = functools.reduce(jnp.add, [jnp.exp(stats[i] - smax) for i in range(N)])
    factor = jnp.exp(mrow[...] - smax) / ssum
    per = 128 // R
    for b in range(N * R // 128):
        bz, bb = divmod(b, G * R // 128)
        spread = jnp.transpose(jnp.broadcast_to(factor[bz][bb : bb + 1, :], (128, 128)))
        for u in range(per):
            t = b * per + u
            for lt in range(Kl // 128):
                lanes = slice(lt * 128, (lt + 1) * 128)
                tbuf[mh, t : t + 1, lanes] = jnp.sum(
                    p[t * R : (t + 1) * R, lanes] * spread[u * R : (u + 1) * R, :], axis=0, keepdims=True
                )
    for i in range(1, NH):
        go(remote(tbuf.at[mh], tbuf.at[mh], ts.at[i], tr.at[mh], head=lax.rem(mh + i, NH)))
    for i in range(1, NH):
        h = lax.rem(mh + i, NH)
        remote(tbuf.at[h], tbuf.at[h], ts.at[0], tr.at[h], head=lax.rem(mh + 1, NH)).wait_recv()
    target = functools.reduce(jnp.add, [tbuf[h] for h in range(NH)]) / H
    dbuf[...] = loss_scale * (dbuf[...] - target)

    def gates(h, own):
        eyej = eye_of(Jl)

        def body(t, carry):
            rows = pl.ds(pl.multiple_of(t * Jl, 8), Jl)
            d = dbuf[pl.ds(t, 1), :]
            wc = wcol[h, rows, :]
            total = jnp.zeros((Jl, 128), f32)
            for lt in range(Kl // 128):
                lanes = slice(lt * 128, (lt + 1) * 128)
                a = act[h, rows, lanes]
                dl = d[:, lanes]
                gate[h, rows, lanes] = jnp.where(a > 0.0, dl * wc, 0.0).astype(bf16)
                if own:
                    total = total + dl * jnp.maximum(a, 0.0)
            if own:
                row = as_row(jnp.sum(total, axis=1, keepdims=True), eyej)
                qpart[lax.rem(t, 2), lax.div(t, 2), Jl : Jl + 8, :] = jnp.broadcast_to(row, (8, 128))
            return carry

        lax.fori_loop(0, Q, body, 0, unroll=4)

    gates(mh, True)
    grads = jnp.dot(gate[mh], ikbuf[...], preferred_element_type=f32) * iscale
    for t in range(Q):
        qpart[t % 2, t // 2, 0:Jl, :] = grads[t * Jl : (t + 1) * Jl]
    pair = remote(qpart.at[1 - core], pairbuf, ps.at[0], pr.at[0], tok=partner)
    go(pair)
    for i in range(1, NH):
        gates(lax.rem(mh + i, NH), False)
    pair.wait_recv()
    rsend[...] = qpart[core] + pairbuf[...]
    for i in range(1, NC):
        other = lax.rem(chip + i, NC)
        go(remote(rsend.at[other], rsbuf.at[chip], rs.at[i], rr.at[chip], tok=other * 2 + core))
    total = jnp.zeros((128, Kl), f32)
    for h in range(NH):
        total = total + lax.dot_general(iqbuf[h], gate[h], (((0,), (0,)), ((), ())), preferred_element_type=f32)
    kg_out[...] = jnp.transpose(total)
    own = rsend[chip]
    for i in range(1, NC):
        src = lax.rem(chip + i, NC)
        remote(rsbuf.at[src], rsbuf.at[src], rs.at[0], rr.at[src], tok=partner).wait_recv()
        own = own + rsbuf[src]
    agbuf[me] = own.astype(bf16)
    for i in range(1, N):
        go(remote(agbuf.at[me], agbuf.at[me], gs.at[i], gr.at[me], tok=lax.rem(me + i, N)))
    for i in range(1, N):
        src = lax.rem(me + i, N)
        remote(agbuf.at[src], agbuf.at[src], gs.at[0], gr.at[src], tok=partner).wait_recv()
    qg_out[...] = agbuf[...]
    for copy in sends:
        copy.wait_send()


def local(queries, latent_keys, index_queries, index_keys, index_weights, positions):
    Hl, _, D = queries.shape
    Kl = latent_keys.shape[0]
    Q, Jl, DI = index_queries.shape
    N = lax.axis_size("tokens")
    NH = lax.axis_size("heads")
    chips = N // 2
    Z = 4 if chips % 4 == 0 else 1
    Y = chips // Z
    R = Hl
    SL = -(-(Jl + 8) // 8) * 8
    loss_scale = float(Kl * N // 8)
    cfg = (NH, N, Z, Y, Q, R, D, Kl, Jl, SL, float(Hl * NH), loss_scale)
    G = 2 * Y
    DMA = pltpu.SemaphoreType.DMA
    any_space = pl.BlockSpec(memory_space=pl.ANY)
    vmem = pl.BlockSpec(memory_space=pltpu.VMEM)
    slabs, keys = pl.pallas_call(
        functools.partial(kernel, cfg),
        out_shape=(
            jax.ShapeDtypeStruct((N, SL, 128), bf16),
            jax.ShapeDtypeStruct((Kl, 128), f32),
        ),
        in_specs=[any_space] * 5 + [pl.BlockSpec(memory_space=pltpu.SMEM)],
        out_specs=(vmem, vmem),
        scratch_shapes=[
            pltpu.VMEM((N, R, D), bf16),
            pltpu.VMEM((Kl, D), bf16),
            pltpu.VMEM((NH, Q * Jl, DI), bf16),
            pltpu.VMEM((Kl, DI), bf16),
            pltpu.VMEM((NH, Q, Jl), f32),
            pltpu.VMEM((NH, Q * Jl, 128), f32),
            pltpu.VMEM((N * R, Kl), f32),
            pltpu.VMEM((NH, Q * Jl, Kl), f32),
            pltpu.VMEM((NH, Q * Jl, Kl), bf16),
            pltpu.VMEM((Q, Kl), f32),
            pltpu.VMEM((Z, G * R // 128, 128), f32),
            pltpu.VMEM((G * R, 1), f32),
            pltpu.VMEM((G * R, 1), f32),
            pltpu.VMEM((N, Z, G * R // 128, 128), f32),
            pltpu.VMEM((N, 8, 128), f32),
            pltpu.VMEM((NH, Q, Kl), f32),
            pltpu.VMEM((Q, Kl), f32),
            pltpu.VMEM((2, chips, SL, 128), f32),
            pltpu.VMEM((chips, SL, 128), f32),
            pltpu.VMEM((chips, SL, 128), f32),
            pltpu.VMEM((chips, SL, 128), f32),
            pltpu.VMEM((N, SL, 128), bf16),
            DMA((5,)),
            DMA((Z,)),
            DMA((Z * Y,)),
            DMA((Z * Y,)),
            DMA((N,)),
            DMA((NH,)),
            DMA((NH,)),
            DMA((NH,)),
            DMA((NH,)),
            DMA((N,)),
            DMA((N,)),
            DMA((N,)),
            DMA((N,)),
            DMA((NH,)),
            DMA((NH,)),
            DMA((1,)),
            DMA((1,)),
            DMA((chips,)),
            DMA((chips,)),
            DMA((N,)),
            DMA((N,)),
        ],
        compiler_params=pltpu.CompilerParams(
            collective_id=0, has_side_effects=True, vmem_limit_bytes=60 * 1024 * 1024
        ),
    )(
        queries.reshape(Hl, D),
        latent_keys,
        index_queries.reshape(Q * Jl, DI),
        index_keys,
        index_weights,
        positions,
    )
    query_grad = slabs[:, :Jl, :].astype(f32)
    weight_grad = slabs[:, Jl, :Jl].astype(f32)
    return (query_grad, weight_grad, keys * (DI ** (-0.5)))


def solution(mesh):
    placed = (
        P("heads", "tokens", None),
        P("tokens", None),
        P(None, "heads", None),
        P("tokens", None),
        P(None, "heads"),
        P(),
    )
    return jax.shard_map(
        local,
        mesh=mesh,
        in_specs=placed,
        out_specs=(P(None, "heads", None), P(None, "heads"), P("tokens", None)),
        check_vma=False,
    )
```

```python
import functools

import jax
import jax.numpy as jnp
from jax import lax
from jax.experimental import pallas as pl
from jax.experimental.pallas import tpu as pltpu
from jax.sharding import PartitionSpec as P

MESH = pl.DeviceIdType.MESH
softmax_scale = 192.0 ** (-0.5)
masked_value = -1e30
open_value = 3e38
f32 = jnp.float32
bf16 = jnp.bfloat16


def swapped(value, step, size):
    if size & (size - 1):
        return lax.rem(value + step, size)
    out = value
    bit = 1
    while bit < size:
        if step & bit:
            out = out + bit - 2 * bit * lax.rem(lax.div(value, bit), 2)
        bit *= 2
    return out


def as_row(column, eye):
    return jnp.sum(jnp.where(eye, column, 0.0), axis=0, keepdims=True)


def eye_of(rows):
    return lax.broadcasted_iota(jnp.int32, (rows, 128), 0) == lax.broadcasted_iota(jnp.int32, (rows, 128), 1)


def kernel(
    cfg, q_in, k_in, iq_in, ik_in, w_in, pos_ref, qg_out, kg_out,
    qbuf, kbuf, iqbuf, ikbuf, wbuf, wcol, p, act, gate, ml, mrow, colm, coll, stats, istats, tbuf, dbuf,
    qpart, pairbuf, rsend, rsbuf, agbuf,
    lsem, zs, ys, cs, qr, hs, hr, ws, wr, ss, sr, iss, isr, ts, tr, ps, pr, rs, rr, gs, gr,
):
    NH, N, Z, Y, Q, R, D, Kl, Jl, SL, H, loss_scale = cfg
    G = 2 * Y
    NC = N // 2
    me = lax.axis_index("tokens")
    mh = lax.axis_index("heads")
    core = lax.rem(me, 2)
    chip = lax.div(me, 2)
    y = lax.rem(chip, Y)
    z = lax.div(chip, Y)
    partner = me + 1 - 2 * core

    def at(zz, yy, cc):
        return (zz * Y + yy) * 2 + cc

    def peer(i):
        return at(swapped(z, i // G, Z), swapped(y, i // 2 % Y, Y), swapped(core, i % 2, 2))

    def remote(src, dst, send, recv, tok=None, head=None):
        device = {"tokens": tok} if head is None else {"heads": head}
        return pltpu.make_async_remote_copy(
            src_ref=src, dst_ref=dst, send_sem=send, recv_sem=recv, device_id=device, device_id_type=MESH
        )

    loads = [
        pltpu.make_async_copy(q_in, qbuf.at[me], lsem.at[0]),
        pltpu.make_async_copy(iq_in, iqbuf.at[mh], lsem.at[1]),
        pltpu.make_async_copy(w_in, wbuf.at[mh], lsem.at[2]),
        pltpu.make_async_copy(ik_in, ikbuf, lsem.at[3]),
        pltpu.make_async_copy(k_in, kbuf, lsem.at[4]),
    ]
    for load in loads:
        load.start()
    barrier = pltpu.get_barrier_semaphore()
    for i in range(1, N):
        pl.semaphore_signal(barrier, inc=1, device_id={"tokens": lax.rem(me + i, N)}, device_id_type=MESH)
    for i in range(1, NH):
        pl.semaphore_signal(barrier, inc=1, device_id={"heads": lax.rem(mh + i, NH)}, device_id_type=MESH)
    for load in loads[:3]:
        load.wait()
    pl.semaphore_wait(barrier, N - 1 + NH - 1)

    sends = []

    def go(copy):
        copy.start()
        sends.append(copy)

    def send_query(src, sem, dest):
        go(remote(qbuf.at[src], qbuf.at[src], sem, qr.at[src], tok=dest))

    def await_query(src):
        remote(qbuf.at[src], qbuf.at[src], zs.at[0], qr.at[src], tok=partner).wait_recv()

    for i in range(1, Z):
        send_query(me, zs.at[i], at(swapped(z, i, Z), y, core))
    for j in range(1, Y):
        send_query(me, ys.at[j], at(z, swapped(y, j, Y), core))
    send_query(me, cs.at[0], partner)
    for i in range(1, NH):
        other = lax.rem(mh + i, NH)
        go(remote(iqbuf.at[mh], iqbuf.at[mh], hs.at[i], hr.at[mh], head=other))
        go(remote(wbuf.at[mh], wbuf.at[mh], ws.at[i], wr.at[mh], head=other))

    key_index = me * Kl + lax.broadcasted_iota(jnp.int32, (1, Kl), 1)
    iscale = 128.0 ** (-0.5)

    def index_part(h):
        wt = jnp.transpose(wbuf[h])
        for t in range(Q):
            wcol[h, t * Jl : (t + 1) * Jl, :] = jnp.broadcast_to(wt[:, t : t + 1], (Jl, 128))
        act[h] = (
            lax.dot_general(iqbuf[h], ikbuf[...], (((1,), (1,)), ((), ())), preferred_element_type=f32) * iscale
        )

    def index_logits(h, first):
        def body(o, carry):
            parts = [[] for _ in range(Kl // 128)]
            for u in range(8):
                rows = pl.ds(pl.multiple_of((o * 8 + u) * Jl, 8), Jl)
                wc = wcol[h, rows, :]
                for lt in range(Kl // 128):
                    a = jnp.maximum(act[h, rows, lt * 128 : (lt + 1) * 128], 0.0)
                    parts[lt].append(jnp.sum(a * wc, axis=0, keepdims=True))
            eight = pl.ds(pl.multiple_of(o * 8, 8), 8)
            for lt in range(Kl // 128):
                lanes = slice(lt * 128, (lt + 1) * 128)
                part = jnp.concatenate(parts[lt], axis=0)
                ml[eight, lanes] = part if first else ml[eight, lanes] + part
            return carry

        lax.fori_loop(0, Q // 8, body, 0)

    eye128 = eye_of(128)

    def score_group(zg):
        group = qbuf[pl.ds(zg * G, G)].reshape(G * R, D)
        base = zg * (G * R)
        scores = lax.dot_general(group, kbuf[...], (((1,), (0,)), ((), ())), preferred_element_type=f32)
        step = min(32, R)
        for i in range(G):
            cap = jnp.where(key_index <= pos_ref[zg * G + i], open_value, masked_value)
            for r in range(0, R, step):
                row = i * R + r
                s = jnp.minimum(scores[row : row + step] * softmax_scale, cap)
                m = jnp.max(s, axis=1, keepdims=True)
                e = jnp.exp(s - m)
                p[pl.ds(pl.multiple_of(base + row, 8), step), :] = e
                colm[row : row + step, :] = m
                coll[row : row + step, :] = m + jnp.log(jnp.sum(e, axis=1, keepdims=True))
        for b in range(G * R // 128):
            mrow[zg, b : b + 1, :] = as_row(colm[b * 128 : (b + 1) * 128, :], eye128)
            stats[me, zg, b : b + 1, :] = as_row(coll[b * 128 : (b + 1) * 128, :], eye128)

    def await_index(h):
        other = lax.rem(mh + 1, NH)
        remote(iqbuf.at[h], iqbuf.at[h], hs.at[0], hr.at[h], head=other).wait_recv()
        remote(wbuf.at[h], wbuf.at[h], ws.at[0], wr.at[h], head=other).wait_recv()

    def index_stats():
        cap = jnp.concatenate(
            [jnp.where(key_index <= pos_ref[t], open_value, masked_value) for t in range(Q)], axis=0
        )
        logits = jnp.minimum(ml[...], cap)
        ml[...] = logits
        imax = jnp.max(logits, axis=1, keepdims=True)
        isum = jnp.sum(jnp.exp(logits - imax), axis=1, keepdims=True)
        istats[me, 0:1, :] = as_row(imax, eyeq)
        istats[me, 1:2, :] = as_row(isum, eyeq)
        for i in range(1, N):
            dst = lax.rem(me + i, N)
            go(remote(istats.at[me], istats.at[me], iss.at[i], isr.at[me], tok=dst))

    def relay_z(i):
        src = at(swapped(z, i, Z), y, core)
        await_query(src)
        for j in range(1, Y):
            send_query(src, ys.at[i * Y + j], at(z, swapped(y, j, Y), core))
        send_query(src, cs.at[i * Y], partner)

    def relay_y(i):
        for j in range(1, Y):
            src = at(swapped(z, i, Z), swapped(y, j, Y), core)
            await_query(src)
            send_query(src, cs.at[i * Y + j], partner)

    def await_pair(i):
        for j in range(Y):
            await_query(at(swapped(z, i, Z), swapped(y, j, Y), 1 - core))

    def index_rest():
        for i in range(1, NH):
            h = lax.rem(mh + i, NH)
            await_index(h)
            index_part(h)
            index_logits(h, False)
        index_stats()

    eyeq = eye_of(Q)
    loads[3].wait()
    index_part(mh)
    index_logits(mh, True)
    relay_y(0)
    loads[4].wait()
    for i in range(1, Z):
        relay_z(i)
        if i == 1:
            await_pair(0)
            score_group(z)
        else:
            relay_y(i - 1)
    index_rest()
    if Z == 1:
        await_pair(0)
        score_group(z)
    else:
        for i in range(1, Z - 1):
            await_pair(i)
            if i == Z - 2:
                relay_y(Z - 1)
            score_group(swapped(z, i, Z))
        if Z == 2:
            relay_y(1)
        await_pair(Z - 1)
        score_group(swapped(z, Z - 1, Z))

    for i in range(1, N):
        go(remote(stats.at[me], stats.at[me], ss.at[i], sr.at[me], tok=peer(N - i)))
    for i in range(1, N):
        src = lax.rem(me + i, N)
        remote(istats.at[src], istats.at[src], iss.at[0], isr.at[src], tok=partner).wait_recv()
    gmax = functools.reduce(jnp.maximum, [istats[i, 0:1, :] for i in range(N)])
    gsum = functools.reduce(jnp.add, [istats[i, 1:2, :] * jnp.exp(istats[i, 0:1, :] - gmax) for i in range(N)])
    gmax_col = jnp.sum(jnp.where(eyeq, gmax, 0.0), axis=1, keepdims=True)
    gsum_col = jnp.sum(jnp.where(eyeq, gsum, 0.0), axis=1, keepdims=True)
    dbuf[...] = jnp.exp(ml[...] - gmax_col) / gsum_col
    for i in range(1, N):
        src = lax.rem(me + i, N)
        remote(stats.at[src], stats.at[src], ss.at[0], sr.at[src], tok=partner).wait_recv()
    smax = functools.reduce(jnp.maximum, [stats[i] for i in range(N)])
    ssum = functools.reduce(jnp.add, [jnp.exp(stats[i] - smax) for i in range(N)])
    factor = jnp.exp(mrow[...] - smax) / ssum
    per = 128 // R
    for b in range(N * R // 128):
        bz, bb = divmod(b, G * R // 128)
        spread = jnp.transpose(jnp.broadcast_to(factor[bz][bb : bb + 1, :], (128, 128)))
        for u in range(per):
            t = b * per + u
            for lt in range(Kl // 128):
                lanes = slice(lt * 128, (lt + 1) * 128)
                tbuf[mh, t : t + 1, lanes] = jnp.sum(
                    p[t * R : (t + 1) * R, lanes] * spread[u * R : (u + 1) * R, :], axis=0, keepdims=True
                )
    for i in range(1, NH):
        go(remote(tbuf.at[mh], tbuf.at[mh], ts.at[i], tr.at[mh], head=lax.rem(mh + i, NH)))
    for i in range(1, NH):
        h = lax.rem(mh + i, NH)
        remote(tbuf.at[h], tbuf.at[h], ts.at[0], tr.at[h], head=lax.rem(mh + 1, NH)).wait_recv()
    target = functools.reduce(jnp.add, [tbuf[h] for h in range(NH)]) / H
    dbuf[...] = loss_scale * (dbuf[...] - target)

    def gates(h, own):
        eyej = eye_of(Jl)

        def body(t, carry):
            rows = pl.ds(pl.multiple_of(t * Jl, 8), Jl)
            d = dbuf[pl.ds(t, 1), :]
            wc = wcol[h, rows, :]
            total = jnp.zeros((Jl, 128), f32)
            for lt in range(Kl // 128):
                lanes = slice(lt * 128, (lt + 1) * 128)
                a = act[h, rows, lanes]
                dl = d[:, lanes]
                gate[h, rows, lanes] = jnp.where(a > 0.0, dl * wc, 0.0).astype(bf16)
                if own:
                    total = total + dl * jnp.maximum(a, 0.0)
            if own:
                row = as_row(jnp.sum(total, axis=1, keepdims=True), eyej)
                qpart[lax.rem(t, 2), lax.div(t, 2), Jl : Jl + 8, :] = jnp.broadcast_to(row, (8, 128))
            return carry

        lax.fori_loop(0, Q, body, 0, unroll=4)

    gates(mh, True)
    grads = jnp.dot(gate[mh], ikbuf[...], preferred_element_type=f32) * iscale
    for t in range(Q):
        qpart[t % 2, t // 2, 0:Jl, :] = grads[t * Jl : (t + 1) * Jl]
    pair = remote(qpart.at[1 - core], pairbuf, ps.at[0], pr.at[0], tok=partner)
    go(pair)
    for i in range(1, NH):
        gates(lax.rem(mh + i, NH), False)
    pair.wait_recv()
    rsend[...] = qpart[core] + pairbuf[...]
    for i in range(NC - 1, 0, -1):
        other = lax.div(peer(2 * i), 2)
        go(remote(rsend.at[other], rsbuf.at[chip], rs.at[i], rr.at[chip], tok=other * 2 + core))
    total = jnp.zeros((128, Kl), f32)
    for h in range(NH):
        total = total + lax.dot_general(iqbuf[h], gate[h], (((0,), (0,)), ((), ())), preferred_element_type=f32)
    kg_out[...] = jnp.transpose(total)
    own = rsend[chip]
    for i in range(1, NC):
        src = lax.rem(chip + i, NC)
        remote(rsbuf.at[src], rsbuf.at[src], rs.at[0], rr.at[src], tok=partner).wait_recv()
        own = own + rsbuf[src]
    agbuf[me] = own.astype(bf16)
    for i in range(N - 1, 0, -1):
        go(remote(agbuf.at[me], agbuf.at[me], gs.at[i], gr.at[me], tok=peer(i)))
    for i in range(1, N):
        src = lax.rem(me + i, N)
        remote(agbuf.at[src], agbuf.at[src], gs.at[0], gr.at[src], tok=partner).wait_recv()
    qg_out[...] = agbuf[...]
    for copy in sends:
        copy.wait_send()


def finish(Jl, scale, slabs, keys, query_grad, weight_grad, key_grad):
    key_grad[...] = keys[...] * scale
    query_grad[...] = slabs[:, 0:Jl, :].astype(f32)
    for t in range(slabs.shape[0]):
        weight_grad[t : t + 1, :] = slabs[t, Jl : Jl + 8, 0:Jl].astype(f32)[0:1]


def local(queries, latent_keys, index_queries, index_keys, index_weights, positions):
    Hl, _, D = queries.shape
    Kl = latent_keys.shape[0]
    Q, Jl, DI = index_queries.shape
    N = lax.axis_size("tokens")
    NH = lax.axis_size("heads")
    chips = N // 2
    Z = 4 if chips % 4 == 0 else 1
    Y = chips // Z
    R = Hl
    SL = -(-(Jl + 8) // 8) * 8
    loss_scale = float(Kl * N // 8)
    cfg = (NH, N, Z, Y, Q, R, D, Kl, Jl, SL, float(Hl * NH), loss_scale)
    G = 2 * Y
    DMA = pltpu.SemaphoreType.DMA
    any_space = pl.BlockSpec(memory_space=pl.ANY)
    vmem = pl.BlockSpec(memory_space=pltpu.VMEM)
    slabs, keys = pl.pallas_call(
        functools.partial(kernel, cfg),
        out_shape=(
            jax.ShapeDtypeStruct((N, SL, 128), bf16),
            jax.ShapeDtypeStruct((Kl, 128), f32),
        ),
        in_specs=[any_space] * 5 + [pl.BlockSpec(memory_space=pltpu.SMEM)],
        out_specs=(vmem, vmem),
        scratch_shapes=[
            pltpu.VMEM((N, R, D), bf16),
            pltpu.VMEM((D, Kl), bf16),
            pltpu.VMEM((NH, Q * Jl, DI), bf16),
            pltpu.VMEM((Kl, DI), bf16),
            pltpu.VMEM((NH, Q, Jl), f32),
            pltpu.VMEM((NH, Q * Jl, 128), f32),
            pltpu.VMEM((N * R, Kl), f32),
            pltpu.VMEM((NH, Q * Jl, Kl), f32),
            pltpu.VMEM((NH, Q * Jl, Kl), bf16),
            pltpu.VMEM((Q, Kl), f32),
            pltpu.VMEM((Z, G * R // 128, 128), f32),
            pltpu.VMEM((G * R, 1), f32),
            pltpu.VMEM((G * R, 1), f32),
            pltpu.VMEM((N, Z, G * R // 128, 128), f32),
            pltpu.VMEM((N, 2, 128), f32),
            pltpu.VMEM((NH, Q, Kl), f32),
            pltpu.VMEM((Q, Kl), f32),
            pltpu.VMEM((2, chips, SL, 128), f32),
            pltpu.VMEM((chips, SL, 128), f32),
            pltpu.VMEM((chips, SL, 128), f32),
            pltpu.VMEM((chips, SL, 128), f32),
            pltpu.VMEM((N, SL, 128), bf16),
            DMA((5,)),
            DMA((Z,)),
            DMA((Z * Y,)),
            DMA((Z * Y,)),
            DMA((N,)),
            DMA((NH,)),
            DMA((NH,)),
            DMA((NH,)),
            DMA((NH,)),
            DMA((N,)),
            DMA((N,)),
            DMA((N,)),
            DMA((N,)),
            DMA((NH,)),
            DMA((NH,)),
            DMA((1,)),
            DMA((1,)),
            DMA((chips,)),
            DMA((chips,)),
            DMA((N,)),
            DMA((N,)),
        ],
        compiler_params=pltpu.CompilerParams(
            collective_id=0, has_side_effects=True, vmem_limit_bytes=60 * 1024 * 1024
        ),
    )(
        queries.reshape(Hl, D),
        latent_keys.T,
        index_queries.reshape(Q * Jl, DI),
        index_keys,
        index_weights,
        positions,
    )
    return pl.pallas_call(
        functools.partial(finish, Jl, DI ** (-0.5)),
        out_shape=(
            jax.ShapeDtypeStruct((Q, Jl, DI), f32),
            jax.ShapeDtypeStruct((Q, Jl), f32),
            jax.ShapeDtypeStruct((Kl, DI), f32),
        ),
        in_specs=[vmem, vmem],
        out_specs=(vmem, vmem, vmem),
    )(slabs, keys)


def solution(mesh):
    placed = (
        P("heads", "tokens", None),
        P("tokens", None),
        P(None, "heads", None),
        P("tokens", None),
        P(None, "heads"),
        P(),
    )
    return jax.shard_map(
        local,
        mesh=mesh,
        in_specs=placed,
        out_specs=(P(None, "heads", None), P(None, "heads"), P("tokens", None)),
        check_vma=False,
    )
```

```python
import functools

import jax
import jax.numpy as jnp
from jax import lax
from jax.experimental import pallas as pl
from jax.experimental.pallas import tpu as pltpu
from jax.sharding import PartitionSpec as P

MESH = pl.DeviceIdType.MESH
softmax_scale = 192.0 ** (-0.5)
masked_value = -1e30
open_value = 3e38
f32 = jnp.float32
bf16 = jnp.bfloat16


def swapped(value, step, size):
    if size & (size - 1):
        return lax.rem(value + step, size)
    out = value
    bit = 1
    while bit < size:
        if step & bit:
            out = out + bit - 2 * bit * lax.rem(lax.div(value, bit), 2)
        bit *= 2
    return out


def as_row(column, eye):
    return jnp.sum(jnp.where(eye, column, 0.0), axis=0, keepdims=True)


def eye_of(rows):
    return lax.broadcasted_iota(jnp.int32, (rows, 128), 0) == lax.broadcasted_iota(jnp.int32, (rows, 128), 1)


def kernel(
    cfg, q_in, k_in, iq_in, ik_in, w_in, pos_ref, qg_out, kg_out,
    qbuf, kbuf, iqbuf, ikbuf, wbuf, wcol, p, act, gate, ml, mrow, colm, coll, stats, istats, tbuf, dbuf,
    qpart, pairbuf, rsend, rsbuf, agbuf,
    lsem, zs, ys, cs, qr, hs, hr, ws, wr, ss, sr, iss, isr, ts, tr, ps, pr, rs, rr, gs, gr,
):
    NH, N, Z, Y, Q, R, D, Kl, Jl, SL, H, loss_scale = cfg
    G = 2 * Y
    NC = N // 2
    me = lax.axis_index("tokens")
    mh = lax.axis_index("heads")
    core = lax.rem(me, 2)
    chip = lax.div(me, 2)
    y = lax.rem(chip, Y)
    z = lax.div(chip, Y)
    partner = me + 1 - 2 * core

    def at(zz, yy, cc):
        return (zz * Y + yy) * 2 + cc

    def peer(i):
        return at(swapped(z, i // G, Z), swapped(y, i // 2 % Y, Y), swapped(core, i % 2, 2))

    def remote(src, dst, send, recv, tok=None, head=None):
        device = {"tokens": tok} if head is None else {"heads": head}
        return pltpu.make_async_remote_copy(
            src_ref=src, dst_ref=dst, send_sem=send, recv_sem=recv, device_id=device, device_id_type=MESH
        )

    loads = [
        pltpu.make_async_copy(q_in, qbuf.at[me], lsem.at[0]),
        pltpu.make_async_copy(iq_in, iqbuf.at[mh], lsem.at[1]),
        pltpu.make_async_copy(w_in, wbuf.at[mh], lsem.at[2]),
        pltpu.make_async_copy(ik_in, ikbuf, lsem.at[3]),
        pltpu.make_async_copy(k_in, kbuf, lsem.at[4]),
    ]
    for load in loads:
        load.start()
    barrier = pltpu.get_barrier_semaphore()
    for i in range(1, N):
        pl.semaphore_signal(barrier, inc=1, device_id={"tokens": lax.rem(me + i, N)}, device_id_type=MESH)
    for i in range(1, NH):
        pl.semaphore_signal(barrier, inc=1, device_id={"heads": lax.rem(mh + i, NH)}, device_id_type=MESH)
    for load in loads[:3]:
        load.wait()
    pl.semaphore_wait(barrier, N - 1 + NH - 1)

    sends = []

    def go(copy):
        copy.start()
        sends.append(copy)

    def send_query(src, sem, dest):
        go(remote(qbuf.at[src], qbuf.at[src], sem, qr.at[src], tok=dest))

    def await_query(src):
        remote(qbuf.at[src], qbuf.at[src], zs.at[0], qr.at[src], tok=partner).wait_recv()

    for i in range(1, Z):
        send_query(me, zs.at[i], at(swapped(z, i, Z), y, core))
    for j in range(1, Y):
        send_query(me, ys.at[j], at(z, swapped(y, j, Y), core))
    send_query(me, cs.at[0], partner)
    for i in range(1, NH):
        other = lax.rem(mh + i, NH)
        go(remote(iqbuf.at[mh], iqbuf.at[mh], hs.at[i], hr.at[mh], head=other))
        go(remote(wbuf.at[mh], wbuf.at[mh], ws.at[i], wr.at[mh], head=other))

    key_index = me * Kl + lax.broadcasted_iota(jnp.int32, (1, Kl), 1)
    iscale = 128.0 ** (-0.5)

    def index_part(h):
        wt = jnp.transpose(wbuf[h])
        for t in range(Q):
            wcol[h, t * Jl : (t + 1) * Jl, :] = jnp.broadcast_to(wt[:, t : t + 1], (Jl, 128))
        act[h] = (
            lax.dot_general(iqbuf[h], ikbuf[...], (((1,), (1,)), ((), ())), preferred_element_type=f32) * iscale
        )

    def index_logits(h, first):
        def body(o, carry):
            parts = [[] for _ in range(Kl // 128)]
            for u in range(8):
                rows = pl.ds(pl.multiple_of((o * 8 + u) * Jl, 8), Jl)
                wc = wcol[h, rows, :]
                for lt in range(Kl // 128):
                    a = jnp.maximum(act[h, rows, lt * 128 : (lt + 1) * 128], 0.0)
                    parts[lt].append(jnp.sum(a * wc, axis=0, keepdims=True))
            eight = pl.ds(pl.multiple_of(o * 8, 8), 8)
            for lt in range(Kl // 128):
                lanes = slice(lt * 128, (lt + 1) * 128)
                part = jnp.concatenate(parts[lt], axis=0)
                ml[eight, lanes] = part if first else ml[eight, lanes] + part
            return carry

        lax.fori_loop(0, Q // 8, body, 0)

    eye128 = eye_of(128)

    def score_group(zg):
        group = qbuf[pl.ds(zg * G, G)].reshape(G * R, D)
        base = zg * (G * R)
        scores = lax.dot_general(group, kbuf[...], (((1,), (0,)), ((), ())), preferred_element_type=f32)
        step = min(32, R)
        for i in range(G):
            cap = jnp.where(key_index <= pos_ref[zg * G + i], open_value, masked_value)
            for r in range(0, R, step):
                row = i * R + r
                s = jnp.minimum(scores[row : row + step] * softmax_scale, cap)
                m = jnp.max(s, axis=1, keepdims=True)
                e = jnp.exp(s - m)
                p[pl.ds(pl.multiple_of(base + row, 8), step), :] = e
                colm[row : row + step, :] = m
                coll[row : row + step, :] = m + jnp.log(jnp.sum(e, axis=1, keepdims=True))
        for b in range(G * R // 128):
            mrow[zg, b : b + 1, :] = as_row(colm[b * 128 : (b + 1) * 128, :], eye128)
            stats[me, zg, b : b + 1, :] = as_row(coll[b * 128 : (b + 1) * 128, :], eye128)

    def await_index(h):
        other = lax.rem(mh + 1, NH)
        remote(iqbuf.at[h], iqbuf.at[h], hs.at[0], hr.at[h], head=other).wait_recv()
        remote(wbuf.at[h], wbuf.at[h], ws.at[0], wr.at[h], head=other).wait_recv()

    def index_stats():
        cap = jnp.concatenate(
            [jnp.where(key_index <= pos_ref[t], open_value, masked_value) for t in range(Q)], axis=0
        )
        logits = jnp.minimum(ml[...], cap)
        ml[...] = logits
        imax = jnp.max(logits, axis=1, keepdims=True)
        isum = jnp.sum(jnp.exp(logits - imax), axis=1, keepdims=True)
        istats[me, 0:1, :] = as_row(imax, eyeq)
        istats[me, 1:2, :] = as_row(isum, eyeq)
        for i in range(1, N):
            dst = lax.rem(me + i, N)
            go(remote(istats.at[me], istats.at[me], iss.at[i], isr.at[me], tok=dst))

    def relay_z(i):
        src = at(swapped(z, i, Z), y, core)
        await_query(src)
        for j in range(1, Y):
            send_query(src, ys.at[i * Y + j], at(z, swapped(y, j, Y), core))
        send_query(src, cs.at[i * Y], partner)

    def relay_y(i):
        for j in range(1, Y):
            src = at(swapped(z, i, Z), swapped(y, j, Y), core)
            await_query(src)
            send_query(src, cs.at[i * Y + j], partner)

    def await_pair(i):
        for j in range(Y):
            await_query(at(swapped(z, i, Z), swapped(y, j, Y), 1 - core))

    eyeq = eye_of(Q)
    loads[3].wait()
    index_part(mh)
    index_logits(mh, True)
    relay_y(0)
    loads[4].wait()
    others = [lax.rem(mh + i, NH) for i in range(1, NH)]

    def other_parts():
        for h in others:
            await_index(h)
            index_part(h)

    def other_logits():
        for h in others:
            index_logits(h, False)
        index_stats()

    if Z == 1:
        other_parts()
        other_logits()
        await_pair(0)
        score_group(z)
    for i in range(1, Z):
        relay_z(i)
        if i == 1:
            await_pair(0)
            score_group(z)
        elif i == 2:
            other_parts()
    for i in range(1, Z):
        relay_y(i)
        if i == 1:
            other_logits()
        else:
            await_pair(i - 1)
            score_group(swapped(z, i - 1, Z))
    if Z > 1:
        await_pair(Z - 1)
        score_group(swapped(z, Z - 1, Z))

    for i in range(1, N):
        go(remote(stats.at[me], stats.at[me], ss.at[i], sr.at[me], tok=peer(N - i)))
    for i in range(1, N):
        src = lax.rem(me + i, N)
        remote(istats.at[src], istats.at[src], iss.at[0], isr.at[src], tok=partner).wait_recv()
    gmax = functools.reduce(jnp.maximum, [istats[i, 0:1, :] for i in range(N)])
    gsum = functools.reduce(jnp.add, [istats[i, 1:2, :] * jnp.exp(istats[i, 0:1, :] - gmax) for i in range(N)])
    gmax_col = jnp.sum(jnp.where(eyeq, gmax, 0.0), axis=1, keepdims=True)
    gsum_col = jnp.sum(jnp.where(eyeq, gsum, 0.0), axis=1, keepdims=True)
    dbuf[...] = jnp.exp(ml[...] - gmax_col) / gsum_col
    for i in range(1, N):
        src = lax.rem(me + i, N)
        remote(stats.at[src], stats.at[src], ss.at[0], sr.at[src], tok=partner).wait_recv()
    smax = functools.reduce(jnp.maximum, [stats[i] for i in range(N)])
    ssum = functools.reduce(jnp.add, [jnp.exp(stats[i] - smax) for i in range(N)])
    factor = jnp.exp(mrow[...] - smax) / ssum
    per = 128 // R
    parts = 2 if Q % 16 == 0 else 1
    QP = Q // parts

    def rows_of(part):
        return pl.ds(part * QP, QP)

    for part in range(parts):
        for b in range(part * QP // per, (part + 1) * QP // per):
            bz, bb = divmod(b, G * R // 128)
            spread = jnp.transpose(jnp.broadcast_to(factor[bz][bb : bb + 1, :], (128, 128)))
            for u in range(per):
                t = b * per + u
                for lt in range(Kl // 128):
                    lanes = slice(lt * 128, (lt + 1) * 128)
                    tbuf[mh, t : t + 1, lanes] = jnp.sum(
                        p[t * R : (t + 1) * R, lanes] * spread[u * R : (u + 1) * R, :], axis=0, keepdims=True
                    )
        for i in range(1, NH):
            block = tbuf.at[mh, rows_of(part)]
            go(remote(block, block, ts.at[part, i], tr.at[part, mh], head=lax.rem(mh + i, NH)))

    def gates(h, own, first, last):
        eyej = eye_of(Jl)

        def body(t, carry):
            rows = pl.ds(pl.multiple_of(t * Jl, 8), Jl)
            d = dbuf[pl.ds(t, 1), :]
            wc = wcol[h, rows, :]
            total = jnp.zeros((Jl, 128), f32)
            for lt in range(Kl // 128):
                lanes = slice(lt * 128, (lt + 1) * 128)
                a = act[h, rows, lanes]
                dl = d[:, lanes]
                gate[h, rows, lanes] = jnp.where(a > 0.0, dl * wc, 0.0).astype(bf16)
                if own:
                    total = total + dl * jnp.maximum(a, 0.0)
            if own:
                row = as_row(jnp.sum(total, axis=1, keepdims=True), eyej)
                qpart[lax.rem(t, 2), lax.div(t, 2), Jl : Jl + 8, :] = jnp.broadcast_to(row, (8, 128))
            return carry

        lax.fori_loop(first, last, body, 0, unroll=4)

    pairs = []
    for part in range(parts):
        for h in others:
            block = tbuf.at[h, rows_of(part)]
            remote(block, block, ts.at[part, 0], tr.at[part, h], head=others[0]).wait_recv()
        rows = slice(part * QP, (part + 1) * QP)
        target = functools.reduce(jnp.add, [tbuf[h, rows, :] for h in range(NH)]) / H
        dbuf[rows, :] = loss_scale * (dbuf[rows, :] - target)
        gates(mh, True, part * QP, (part + 1) * QP)
        grads = (
            jnp.dot(gate[mh, part * QP * Jl : (part + 1) * QP * Jl, :], ikbuf[...], preferred_element_type=f32)
            * iscale
        )
        for i in range(QP):
            t = part * QP + i
            qpart[t % 2, t // 2, 0:Jl, :] = grads[i * Jl : (i + 1) * Jl]
        span = pl.ds(part * QP // 2, QP // 2)
        pairs.append(
            remote(qpart.at[1 - core, span], pairbuf.at[span], ps.at[part], pr.at[part], tok=partner)
        )
        go(pairs[-1])
    for h in others:
        gates(h, False, 0, Q)
    for pair in pairs:
        pair.wait_recv()
    rsend[...] = qpart[core] + pairbuf[...]
    for i in range(NC - 1, 0, -1):
        other = lax.div(peer(2 * i), 2)
        go(remote(rsend.at[other], rsbuf.at[chip], rs.at[i], rr.at[chip], tok=other * 2 + core))
    total = jnp.zeros((128, Kl), f32)
    for h in range(NH):
        total = total + lax.dot_general(iqbuf[h], gate[h], (((0,), (0,)), ((), ())), preferred_element_type=f32)
    kg_out[...] = jnp.transpose(total)
    own = rsend[chip]
    for i in range(1, NC):
        src = lax.rem(chip + i, NC)
        remote(rsbuf.at[src], rsbuf.at[src], rs.at[0], rr.at[src], tok=partner).wait_recv()
        own = own + rsbuf[src]
    agbuf[me] = own.astype(bf16)
    for i in range(NC - 1, 0, -1):
        go(remote(agbuf.at[me], agbuf.at[me], gs.at[2 * i], gr.at[me], tok=peer(2 * i)))
    go(remote(agbuf.at[me], agbuf.at[me], gs.at[1], gr.at[me], tok=partner))

    def await_slab(src):
        remote(agbuf.at[src], agbuf.at[src], gs.at[0], gr.at[src], tok=partner).wait_recv()

    for i in range(1, NC):
        src = peer(2 * i)
        await_slab(src)
        go(remote(agbuf.at[src], agbuf.at[src], gs.at[2 * i + 1], gr.at[src], tok=partner))
    for i in range(NC):
        await_slab(peer(2 * i + 1))
    qg_out[...] = agbuf[...]
    for copy in sends:
        copy.wait_send()


def finish(Jl, scale, slabs, keys, query_grad, weight_grad, key_grad):
    key_grad[...] = keys[...] * scale
    query_grad[...] = slabs[:, 0:Jl, :].astype(f32)
    for t in range(slabs.shape[0]):
        weight_grad[t : t + 1, :] = slabs[t, Jl : Jl + 8, 0:Jl].astype(f32)[0:1]


def local(queries, latent_keys, index_queries, index_keys, index_weights, positions):
    Hl, _, D = queries.shape
    Kl = latent_keys.shape[0]
    Q, Jl, DI = index_queries.shape
    N = lax.axis_size("tokens")
    NH = lax.axis_size("heads")
    chips = N // 2
    Z = 4 if chips % 4 == 0 else 1
    Y = chips // Z
    R = Hl
    SL = -(-(Jl + 8) // 8) * 8
    loss_scale = float(Kl * N // 8)
    cfg = (NH, N, Z, Y, Q, R, D, Kl, Jl, SL, float(Hl * NH), loss_scale)
    G = 2 * Y
    DMA = pltpu.SemaphoreType.DMA
    any_space = pl.BlockSpec(memory_space=pl.ANY)
    vmem = pl.BlockSpec(memory_space=pltpu.VMEM)
    slabs, keys = pl.pallas_call(
        functools.partial(kernel, cfg),
        out_shape=(
            jax.ShapeDtypeStruct((N, SL, 128), bf16),
            jax.ShapeDtypeStruct((Kl, 128), f32),
        ),
        in_specs=[any_space] * 5 + [pl.BlockSpec(memory_space=pltpu.SMEM)],
        out_specs=(vmem, vmem),
        scratch_shapes=[
            pltpu.VMEM((N, R, D), bf16),
            pltpu.VMEM((D, Kl), bf16),
            pltpu.VMEM((NH, Q * Jl, DI), bf16),
            pltpu.VMEM((Kl, DI), bf16),
            pltpu.VMEM((NH, Q, Jl), f32),
            pltpu.VMEM((NH, Q * Jl, 128), f32),
            pltpu.VMEM((N * R, Kl), f32),
            pltpu.VMEM((NH, Q * Jl, Kl), f32),
            pltpu.VMEM((NH, Q * Jl, Kl), bf16),
            pltpu.VMEM((Q, Kl), f32),
            pltpu.VMEM((Z, G * R // 128, 128), f32),
            pltpu.VMEM((G * R, 1), f32),
            pltpu.VMEM((G * R, 1), f32),
            pltpu.VMEM((N, Z, G * R // 128, 128), f32),
            pltpu.VMEM((N, 2, 128), f32),
            pltpu.VMEM((NH, Q, Kl), f32),
            pltpu.VMEM((Q, Kl), f32),
            pltpu.VMEM((2, chips, SL, 128), f32),
            pltpu.VMEM((chips, SL, 128), f32),
            pltpu.VMEM((chips, SL, 128), f32),
            pltpu.VMEM((chips, SL, 128), f32),
            pltpu.VMEM((N, SL, 128), bf16),
            DMA((5,)),
            DMA((Z,)),
            DMA((Z * Y,)),
            DMA((Z * Y,)),
            DMA((N,)),
            DMA((NH,)),
            DMA((NH,)),
            DMA((NH,)),
            DMA((NH,)),
            DMA((N,)),
            DMA((N,)),
            DMA((N,)),
            DMA((N,)),
            DMA((2, NH)),
            DMA((2, NH)),
            DMA((2,)),
            DMA((2,)),
            DMA((chips,)),
            DMA((chips,)),
            DMA((N,)),
            DMA((N,)),
        ],
        compiler_params=pltpu.CompilerParams(
            collective_id=0, has_side_effects=True, vmem_limit_bytes=60 * 1024 * 1024
        ),
    )(
        queries.reshape(Hl, D),
        latent_keys.T,
        index_queries.reshape(Q * Jl, DI),
        index_keys,
        index_weights,
        positions,
    )
    return pl.pallas_call(
        functools.partial(finish, Jl, DI ** (-0.5)),
        out_shape=(
            jax.ShapeDtypeStruct((Q, Jl, DI), f32),
            jax.ShapeDtypeStruct((Q, Jl), f32),
            jax.ShapeDtypeStruct((Kl, DI), f32),
        ),
        in_specs=[vmem, vmem],
        out_specs=(vmem, vmem, vmem),
    )(slabs, keys)


def solution(mesh):
    placed = (
        P("heads", "tokens", None),
        P("tokens", None),
        P(None, "heads", None),
        P("tokens", None),
        P(None, "heads"),
        P(),
    )
    return jax.shard_map(
        local,
        mesh=mesh,
        in_specs=placed,
        out_specs=(P(None, "heads", None), P(None, "heads"), P("tokens", None)),
        check_vma=False,
    )
```
